64 devices in a mesh: dp: 4 (over x, y), fsdp: 16 (over z, core).
Axes of the slice: x: 2, y: 2, z: 8, core: 2. Of those that a mesh axis runs over, the one named last changes fastest.
The devices are a block of a 4x4x8 slice.
Arguments:
- x: bfloat16 [64, 1024, 1152], P(('dp', 'fsdp')), parts along dimension 0
- w_q: bfloat16 [2, 1152, 1024], P(None, 'fsdp')
- w_k: bfloat16 [2, 1152, 256], P(None, 'fsdp')
- w_v: bfloat16 [2, 1152, 256], P(None, 'fsdp')
- w_o: bfloat16 [2, 1024, 1152], P(None, 'fsdp')
- w_gate: bfloat16 [2, 1152, 6912], P(None, 'fsdp')
- w_up: bfloat16 [2, 1152, 6912], P(None, 'fsdp')
- w_down: bfloat16 [2, 6912, 1152], P(None, 'fsdp')
- norm_w: float32 [2, 4, 1152], replicated
- qk_norm_w: float32 [2, 2, 256], replicated
Outputs:
- output 1: bfloat16 [64, 1024, 1152], P(('dp', 'fsdp')), parts along dimension 0
- output 2: bfloat16 [64, 1024, 1, 256], P(('dp', 'fsdp')), parts along dimension 0
- output 3: bfloat16 [64, 1024, 1, 256], P(('dp', 'fsdp')), parts along dimension 0
There are 4 independent parts. The reference program is written for one: setup_inputs(seed, part) draws one part's arguments, and reference() takes and returns one part's arrays. A program takes and returns all parts, laid end to end along the dimension named above; an argument that names none is the same for every part.
All inputs are finite; a program needn't handle non-finite values.
Results may differ from the reference program's by a relative error of at most 0.0142371.
Values are sent between devices in bfloat16 or wider.
A program may use at most 768 MiB of HBM per device.

```python
import jax
import jax.numpy as jnp
from jax import lax

MODEL_DIM = 1152
NUM_HEADS = 4
KV_HEADS = 1
HEAD_DIM = 256
FFN_DIM = 6912
WINDOW = 1024
NUM_SEQS = 16
SEQ_LEN = 1024

NORM_EPS = 1e-6
LOCAL_BASE = 10000.0
GLOBAL_BASE = 1000000.0
GLOBAL_POS_DIV = 8.0


def setup_inputs(seed: int = 0, part: int = 0) -> dict:
    base_key = jax.random.key(seed)
    sub_keys = jax.random.split(base_key, 10)
    x_key = jax.random.fold_in(sub_keys[0], part)
    q_width = NUM_HEADS * HEAD_DIM
    kv_width = KV_HEADS * HEAD_DIM

    def draw_weight(rand_key, fan_in, fan_out):
        values = jax.random.normal(rand_key, (2, fan_in, fan_out), jnp.float32) * fan_in ** -0.5
        return values.astype(jnp.bfloat16)

    return {
        'x': jax.random.normal(x_key, (NUM_SEQS, SEQ_LEN, MODEL_DIM), jnp.float32).astype(jnp.bfloat16),
        'w_q': draw_weight(sub_keys[1], MODEL_DIM, q_width),
        'w_k': draw_weight(sub_keys[2], MODEL_DIM, kv_width),
        'w_v': draw_weight(sub_keys[3], MODEL_DIM, kv_width),
        'w_o': draw_weight(sub_keys[4], q_width, MODEL_DIM),
        'w_gate': draw_weight(sub_keys[5], MODEL_DIM, FFN_DIM),
        'w_up': draw_weight(sub_keys[6], MODEL_DIM, FFN_DIM),
        'w_down': draw_weight(sub_keys[7], FFN_DIM, MODEL_DIM),
        'norm_w': 0.3 * jax.random.normal(sub_keys[8], (2, 4, MODEL_DIM), jnp.float32),
        'qk_norm_w': 0.3 * jax.random.normal(sub_keys[9], (2, 2, HEAD_DIM), jnp.float32),
    }


def rms_norm(values, gain_w):
    mean_sq = jnp.mean(values * values, axis=-1, keepdims=True)
    return values * lax.rsqrt(mean_sq + NORM_EPS) * (1.0 + gain_w)


def rope_tables(rope_base, pos_div):
    half_dim = HEAD_DIM // 2
    inv_freq = rope_base ** (-2.0 * jnp.arange(half_dim, dtype=jnp.float32) / HEAD_DIM)
    positions = jnp.arange(SEQ_LEN, dtype=jnp.float32) / pos_div
    angles = positions[:, None] * inv_freq[None, :]
    return jnp.cos(angles), jnp.sin(angles)


def apply_rope(values, cos_t, sin_t):
    half_dim = values.shape[-1] // 2
    lo_half = values[..., :half_dim]
    hi_half = values[..., half_dim:]
    cos_b = cos_t[:, None, :]
    sin_b = sin_t[:, None, :]
    return jnp.concatenate([lo_half * cos_b - hi_half * sin_b, hi_half * cos_b + lo_half * sin_b], axis=-1)


def attend(query_bf, key_bf, value_bf, window):
    groups = NUM_HEADS // KV_HEADS
    q_scalar = MODEL_DIM // NUM_HEADS if HEAD_DIM == 128 else HEAD_DIM
    q_scale = q_scalar ** -0.5
    q_block = min(SEQ_LEN, 512)
    num_blocks = SEQ_LEN // q_block
    query_grp = query_bf.astype(jnp.float32).reshape(num_blocks, q_block, KV_HEADS, groups, HEAD_DIM)
    key_f32 = key_bf.astype(jnp.float32)
    value_f32 = value_bf.astype(jnp.float32)
    key_pos = jnp.arange(SEQ_LEN)

    def one_block(block_args):
        blk_idx, q_blk = block_args
        q_pos = blk_idx * q_block + jnp.arange(q_block)
        scores = jnp.einsum('qkgd,skd->kgqs', q_blk, key_f32) * q_scale
        pos_diff = q_pos[:, None] - key_pos[None, :]
        allowed = (pos_diff >= 0) & (pos_diff < window)
        scores = jnp.where(allowed, scores, -1e30)
        probs_bf = jax.nn.softmax(scores, axis=-1).astype(jnp.bfloat16)
        block_out = jnp.einsum('kgqs,skd->qkgd', probs_bf.astype(jnp.float32), value_f32)
        return block_out.astype(jnp.bfloat16)

    block_outs = lax.map(one_block, (jnp.arange(num_blocks), query_grp))
    return block_outs.reshape(SEQ_LEN, NUM_HEADS * HEAD_DIM)


def decoder_layer(x_seq, weights, norm_w, qk_norm_w, window, rope_base, pos_div):
    w_q, w_k, w_v, w_o, w_gate, w_up, w_down = weights
    x_f32 = x_seq.astype(jnp.float32)
    normed = rms_norm(x_f32, norm_w[0]).astype(jnp.bfloat16)
    query_f32 = jnp.dot(normed, w_q, preferred_element_type=jnp.float32).reshape(SEQ_LEN, NUM_HEADS, HEAD_DIM)
    key_f32 = jnp.dot(normed, w_k, preferred_element_type=jnp.float32).reshape(SEQ_LEN, KV_HEADS, HEAD_DIM)
    value_bf = jnp.dot(normed, w_v, preferred_element_type=jnp.float32).astype(jnp.bfloat16).reshape(SEQ_LEN, KV_HEADS, HEAD_DIM)
    cos_t, sin_t = rope_tables(rope_base, pos_div)
    query_bf = apply_rope(rms_norm(query_f32, qk_norm_w[0]), cos_t, sin_t).astype(jnp.bfloat16)
    key_bf = apply_rope(rms_norm(key_f32, qk_norm_w[1]), cos_t, sin_t).astype(jnp.bfloat16)
    attn_out = attend(query_bf, key_bf, value_bf, window)
    attn_proj = jnp.dot(attn_out, w_o, preferred_element_type=jnp.float32)
    resid = (x_f32 + rms_norm(attn_proj, norm_w[1])).astype(jnp.bfloat16)
    resid_f32 = resid.astype(jnp.float32)
    normed_ffn = rms_norm(resid_f32, norm_w[2]).astype(jnp.bfloat16)
    gate_f32 = jnp.dot(normed_ffn, w_gate, preferred_element_type=jnp.float32)
    up_f32 = jnp.dot(normed_ffn, w_up, preferred_element_type=jnp.float32)
    hidden_act = (jax.nn.gelu(gate_f32, approximate=True) * up_f32).astype(jnp.bfloat16)
    down_f32 = jnp.dot(hidden_act, w_down, preferred_element_type=jnp.float32)
    layer_out = (resid_f32 + rms_norm(down_f32, norm_w[3])).astype(jnp.bfloat16)
    return layer_out, key_bf, value_bf


def reference(x, w_q, w_k, w_v, w_o, w_gate, w_up, w_down, norm_w, qk_norm_w):
    stacked = (w_q, w_k, w_v, w_o, w_gate, w_up, w_down)
    local_w = tuple(w_all[0] for w_all in stacked)
    global_w = tuple(w_all[1] for w_all in stacked)

    def one_seq(x_seq):
        hidden = decoder_layer(x_seq, local_w, norm_w[0], qk_norm_w[0], WINDOW, LOCAL_BASE, 1.0)[0]
        return decoder_layer(hidden, global_w, norm_w[1], qk_norm_w[1], SEQ_LEN, GLOBAL_BASE, GLOBAL_POS_DIV)

    x_out, k_cache, v_cache = lax.map(one_seq, x)
    return (x_out, k_cache, v_cache)
```

```python
import functools
import math

import jax
import jax.numpy as jnp
from jax import lax
from jax.experimental import pallas as pl
from jax.experimental.pallas import tpu as pltpu
from jax.sharding import PartitionSpec as P

WINDOW = 1024
NORM_EPS = 1e-6
ROPE_BASES = (10000.0, 1000000.0)
ROPE_DIVS = (1.0, 8.0)
MESH = pl.DeviceIdType.MESH
LANES = 128
DELTA = 2
SLOTS = 8
PIECES = 4


class Comm:
    def __init__(self, side, nz, ng, s_ref, g_ref, ssem, rsem, lsem):
        self.ng, self.nz, self.s, self.g = ng, nz, s_ref, g_ref
        self.ssem, self.rsem, self.lsem = ssem, rsem, lsem
        d, f = lax.axis_index("dp"), lax.axis_index("fsdp")
        self.z, self.c = f // 2, f % 2
        xi, yi = d // side, d % side
        a, b = xi % 2, yi % 2
        self.h = (a + b) % 2
        self.up = {"dp": d, "fsdp": ((self.z + 1) % nz) * 2 + self.c}
        self.down = {"dp": d, "fsdp": ((self.z + nz - 1) % nz) * 2 + self.c}
        self.sib = {"dp": d, "fsdp": self.z * 2 + 1 - self.c}
        self.over_x = {"dp": (xi + 1 - 2 * a) * side + yi, "fsdp": f}
        self.over_y = {"dp": xi * side + yi + 1 - 2 * b, "fsdp": f}
        self.hops = nz // 2
        self.stages = self.hops + 2

    def barrier(self):
        bar = pltpu.get_barrier_semaphore()
        peers = (self.up, self.down, self.sib, self.over_x, self.over_y)
        for peer in peers:
            pl.semaphore_signal(bar, inc=1, device_id=peer, device_id_type=MESH)
        pl.semaphore_wait(bar, len(peers))

    def copies(self, k, g, slot):
        rows, nz, n = self.s.shape[2], self.nz, 2 * self.hops
        mine = pl.ds(pl.multiple_of(self.c * rows, 8), rows)

        def remote(i, src, dst, peer):
            return pltpu.make_async_remote_copy(
                src_ref=src, dst_ref=dst, send_sem=self.ssem.at[i, slot], recv_sem=self.rsem.at[i, slot],
                device_id=peer, device_id_type=MESH)

        if k < self.hops:
            half = k == self.hops - 1
            pu = pl.ds(2 * self.h, 1 if half else 2)
            pd = pl.ds(2 * self.h + 1, 1) if half else pu
            if k == 0:
                su, sd = self.s.at[g, pu], self.s.at[g, pd]
            else:
                su, sd = self.g.at[g, pu, nz - k, mine], self.g.at[g, pd, k, mine]
            out = [remote(2 * k, su, self.g.at[g, pu, nz - 1 - k, mine], self.up),
                   remote(2 * k + 1, sd, self.g.at[g, pd, k + 1, mine], self.down)]
            if k == 0:
                out.append(remote(n + 3, self.s.at[g], self.g.at[g, :, 0, mine], self.sib))
            return out
        rest = pl.ds(1, nz - 1)
        if k == self.hops:
            p = 2 * self.h
            px, py = self.g.at[g, p, rest, mine], self.g.at[g, p + 1, rest, mine]
            return [remote(n, px, px, self.over_x), remote(n + 1, py, py, self.over_y)]
        both = self.g.at[g, :, rest, mine]
        return [remote(n + 2, both, both, self.sib)]

    def own(self, g, slot):
        rows = self.s.shape[2]
        mine = pl.ds(pl.multiple_of(self.c * rows, 8), rows)
        return pltpu.make_async_copy(self.s.at[g], self.g.at[g, :, 0, mine], self.lsem.at[slot])

    def tick(self, t):
        slot, old = t % SLOTS, (t + SLOTS - DELTA) % SLOTS

        @pl.when(t < self.ng)
        def _():
            for cp in self.copies(0, t, slot):
                cp.start()
            self.own(t, slot).start()

        for k in range(1, self.stages + 1):
            g = t - DELTA * k

            @pl.when((g >= 0) & (g < self.ng))
            def _(k=k, g=g):
                for cp in self.copies(k - 1, g, old):
                    cp.wait()
                if k == 1:
                    self.own(g, old).wait()
                if k < self.stages:
                    for cp in self.copies(k, g, slot):
                        cp.start()

    def ticks(self, first, count):
        def body(i, carry):
            self.tick(first + i)
            return carry
        lax.fori_loop(0, count, body, 0)


def rms(values, gain):
    mean_sq = jnp.mean(values * values, axis=-1, keepdims=True)
    return values * lax.rsqrt(mean_sq + NORM_EPS) * (1.0 + gain)


def rope(values, cos_t, sin_t):
    half = values.shape[-1] // 2
    lo, hi = values[:, :half], values[:, half:]
    return jnp.concatenate([lo * cos_t - hi * sin_t, hi * cos_t + lo * sin_t], axis=-1)


def dot(a, b):
    return jnp.dot(a, b, preferred_element_type=jnp.float32)


def kernel(cfg, x_hbm, nw, qkn, tab, s_hbm, xo_hbm, ko_hbm, vo_hbm, g_hbm,
           xs, hs, x1, qs, ks, vs, at, ob, us, ys, wb, db,
           ssem, rsem, lsem, wsem, osem, dsem, iosem):
    side, nz, ng, layers, heads, hd, nf, nd, scale = cfg
    seq, dm = xs.shape
    rows_o = ob.shape[1] // (2 * nz)
    rows_d = db.shape[2] // (2 * nz)
    rows = s_hbm.shape[2]
    nsub = rows_d // rows
    ncol = dm // LANES
    per = ng // layers
    cm = Comm(side, nz, ng, s_hbm, g_hbm, ssem, rsem, lsem)
    cm.barrier()
    load_x = pltpu.make_async_copy(x_hbm, xs, iosem.at[0])
    load_x.start()
    lead = DELTA * cm.stages + 1
    first = lead + 2
    g_qkv, g_o, g_f, g_d = 0, 3, 6, 6 + nf
    MB = 256

    def place(rel):
        return (cm.z + rel) % nz

    def load_w(g, slot):
        for rel in range(nz):
            dst = wb.at[slot, :, pl.ds(pl.multiple_of(place(rel) * 2 * rows, 16), 2 * rows), :]
            pltpu.make_async_copy(g_hbm.at[g, :, rel], dst, wsem.at[slot]).start()

    def wait_w(slot):
        pltpu.make_async_copy(wb.at[slot], wb.at[slot], wsem.at[slot]).wait()

    def load_o(base):
        for i in range(pl.cdiv(ncol, PIECES)):
            n = min(PIECES, ncol - PIECES * i)
            for rel in range(nz):
                for c in range(2):
                    src = g_hbm.at[base + g_o + i, pl.ds(0, n), rel, pl.ds(c * rows, rows_o), :]
                    off = pl.multiple_of((place(rel) * 2 + c) * rows_o, 16)
                    dst = ob.at[pl.ds(PIECES * i, n), pl.ds(off, rows_o), :]
                    pltpu.make_async_copy(src, dst, osem.at[0]).start()

    def wait_o():
        pltpu.make_async_copy(ob, ob, osem.at[0]).wait()

    def load_d(base, batch, slot):
        for r in range(nsub):
            for rel in range(nz):
                for c in range(2):
                    src = g_hbm.at[base + g_d + batch * nsub + r, :, rel, pl.ds(c * rows, rows), :]
                    off = pl.multiple_of((place(rel) * 2 + c) * rows_d + r * rows, 8)
                    dst = db.at[slot, :, pl.ds(off, rows), :]
                    pltpu.make_async_copy(src, dst, dsem.at[slot]).start()

    def wait_d(slot):
        pltpu.make_async_copy(db.at[slot], db.at[slot], dsem.at[slot]).wait()

    def load_tail(base, slot):
        for r in range(nsub):
            for rel in range(nz):
                for c in range(2):
                    g = base + g_d + (ncol // PIECES) * nsub + r // PIECES
                    src = g_hbm.at[g, r % PIECES, rel, pl.ds(c * rows, rows), :]
                    off = pl.multiple_of((place(rel) * 2 + c) * rows_d + r * rows, 8)
                    dst = db.at[slot, 0, pl.ds(off, rows), :]
                    pltpu.make_async_copy(src, dst, dsem.at[slot]).start()

    def wait_tail(slot):
        pltpu.make_async_copy(db.at[slot, 0], db.at[slot, 0], dsem.at[slot]).wait()

    def blocks(n, size, body):
        def step(i, carry):
            body(i, pl.ds(pl.multiple_of(i * size, size), size))
            return carry
        lax.fori_loop(0, n // size, step, 0)

    cm.ticks(0, 1)
    load_x.wait()

    def norm_in(i, r):
        hs[r, :] = rms(xs[r, :].astype(jnp.float32), nw[0, pl.ds(0, 1), :]).astype(jnp.bfloat16)
    blocks(seq, MB, norm_in)
    cm.ticks(1, first - 1)

    def pair(ref, p):
        return jnp.concatenate([ref[2 * p], ref[2 * p + 1]], axis=-1)

    def layer(l, carry):
        base = l * per
        t0 = base + first

        load_w(base, 0)

        def head_out(r, acc, which):
            out = rms(acc, qkn[l, pl.ds(which, 1), :])
            return rope(out, tab[l, 0, r, :], tab[l, 1, r, :]).astype(jnp.bfloat16)

        for i in range(2):
            load_w(base + i + 1, (i + 1) % 2)
            wait_w(i % 2)

            def q_block(j, r, i=i):
                for p in range(2):
                    qs[2 * i + p, r, :] = head_out(r, dot(hs[r, :], pair(wb.at[i % 2], p)), 0)
            blocks(seq, MB, q_block)
            cm.tick(t0 + i)
        wait_w(0)

        def kv_block(j, r):
            ks[r, :] = head_out(r, dot(hs[r, :], pair(wb.at[0], 0)), 1)
            vs[r, :] = dot(hs[r, :], pair(wb.at[0], 1)).astype(jnp.bfloat16)
        blocks(seq, MB, kv_block)
        cm.tick(t0 + 2)
        load_o(base)
        done = 3

        @pl.when(l == layers - 1)
        def _():
            pltpu.make_async_copy(ks, ko_hbm, iosem.at[1]).start()
            pltpu.make_async_copy(vs, vo_hbm, iosem.at[2]).start()

        nb = seq // MB
        for b in range(nb):
            r = pl.ds(b * MB, MB)
            span = (b + 1) * MB
            per_tick = heads if b < nb // 2 else heads // 2

            def one_head(j, b=b, r=r, span=span):
                sc = lax.dot_general(qs[j, r, :], ks[pl.ds(0, span), :], (((1,), (1,)), ((), ())),
                                     preferred_element_type=jnp.float32) * scale
                diff = (b * MB + lax.broadcasted_iota(jnp.int32, sc.shape, 0)
                        - lax.broadcasted_iota(jnp.int32, sc.shape, 1))
                allowed = diff >= 0
                if span > WINDOW:
                    allowed = allowed & ((diff < WINDOW) | (l > 0))
                sc = jnp.where(allowed, sc, -1e30)
                e = jnp.exp(sc - jnp.max(sc, axis=-1, keepdims=True))
                probs = (e * (1.0 / jnp.sum(e, axis=-1, keepdims=True))).astype(jnp.bfloat16)
                at[j, r, :] = dot(probs, vs[pl.ds(0, span), :]).astype(jnp.bfloat16)

            for first_head in range(0, heads, per_tick):
                def body(j, carry):
                    one_head(j)
                    return carry
                lax.fori_loop(first_head, first_head + per_tick, body, 0)
                cm.tick(t0 + done)
                done += 1

        load_w(base + g_f, 0)
        wait_o()

        def o_block(i, r):
            lhs = jnp.concatenate([at[j, r, :] for j in range(heads)], axis=-1)
            parts = [dot(lhs, pair(ob, p)) for p in range(ncol // 2)]
            if ncol % 2:
                parts.append(dot(lhs, ob[ncol - 1]))
            proj = jnp.concatenate(parts, axis=-1)
            res = (xs[r, :].astype(jnp.float32) + rms(proj, nw[l, pl.ds(1, 1), :])).astype(jnp.bfloat16)
            x1[r, :] = res
            hs[r, :] = rms(res.astype(jnp.float32), nw[l, pl.ds(2, 1), :]).astype(jnp.bfloat16)
        blocks(seq, MB, o_block)
        cm.ticks(t0 + done, 2)
        done += 2

        def gu(j, slot, last=False):
            if not last:
                load_w(base + g_f + j + 1, 1 - slot)
            wait_w(slot)

            def block(i, r):
                gate, up = dot(hs[r, :], pair(wb.at[slot], 0)), dot(hs[r, :], pair(wb.at[slot], 1))
                us[j, r, :] = (jax.nn.gelu(gate, approximate=True) * up).astype(jnp.bfloat16)
            blocks(seq, 2 * MB, block)

        fast = 6
        def two(i, carry):
            gu(2 * i, 0)
            gu(2 * i + 1, 1)
            cm.tick(t0 + done + i)
            return carry
        lax.fori_loop(0, fast, two, 0)
        done += fast

        def one(i, carry):
            gu(2 * fast + i, i % 2)
            cm.tick(t0 + done + i)
            return carry
        singles = nf - 1 - 2 * fast
        lax.fori_loop(0, singles, one, 0)
        done += singles
        gu(nf - 1, (nf - 1) % 2, last=True)

        def lhs_u(r):
            return jnp.concatenate([us[j, r, :] for j in range(nf)], axis=-1)

        need = g_d + nsub + lead - 1 - first
        cm.ticks(t0 + done, need - done)
        done = need
        nbatch = ncol // PIECES
        load_d(base, 0, 0)
        for b in range(nbatch):
            wait_d(b % 2)
            count = nsub if b + 1 < nbatch else pl.cdiv(nsub, PIECES)
            steps = (PIECES // 2) * (seq // MB)

            def d_step(i, carry, b=b):
                p, m = i // (seq // MB), i % (seq // MB)
                r = pl.ds(pl.multiple_of(m * MB, MB), MB)
                w = jnp.concatenate([db[b % 2, 2 * p], db[b % 2, 2 * p + 1]], axis=-1)
                ys[2 * b + p, r, :] = dot(lhs_u(r), w)
                return carry

            def d_tick(i, carry, done=done):
                d_step(i, 0)
                cm.tick(t0 + done + i)
                return carry
            lax.fori_loop(0, count, d_tick, 0)
            done += count
            if b + 1 < nbatch:
                load_d(base, b + 1, (b + 1) % 2)
            else:
                load_tail(base, (b + 1) % 2)
            lax.fori_loop(count, steps, d_step, 0)
        wait_tail(nbatch % 2)

        def fin(i, r):
            tail = dot(lhs_u(r), db[nbatch % 2, 0])
            down = jnp.concatenate([ys[p, r, :] for p in range(ncol // 2)] + [tail], axis=-1)
            res = (x1[r, :].astype(jnp.float32) + rms(down, nw[l, pl.ds(3, 1), :])).astype(jnp.bfloat16)
            xs[r, :] = res
            nxt = jnp.minimum(l + 1, layers - 1)
            hs[r, :] = rms(res.astype(jnp.float32), nw[nxt, pl.ds(0, 1), :]).astype(jnp.bfloat16)
        blocks(seq, MB, fin)
        cm.ticks(t0 + done, per - done)
        return carry

    lax.fori_loop(0, layers, layer, 0)
    out = pltpu.make_async_copy(xs, xo_hbm, iosem.at[0])
    out.start()
    pltpu.make_async_copy(ks, ko_hbm, iosem.at[1]).wait()
    pltpu.make_async_copy(vs, vo_hbm, iosem.at[2]).wait()
    out.wait()


def rope_tables(seq_len, head_dim, rope_base, pos_div):
    half_dim = head_dim // 2
    inv_freq = rope_base ** (-2.0 * jnp.arange(half_dim, dtype=jnp.float32) / head_dim)
    positions = jnp.arange(seq_len, dtype=jnp.float32) / pos_div
    angles = positions[:, None] * inv_freq[None, :]
    return jnp.stack([jnp.cos(angles), jnp.sin(angles)])


def units(rows, l, w_q, w_k, w_v, w_o, w_gate, w_up, w_down):
    def cols(w):
        return w.reshape(w.shape[0], -1, LANES).transpose(1, 0, 2)

    def padded(w, n):
        return jnp.pad(w, ((0, -w.shape[0] % n), (0, 0), (0, 0)))

    qkv = jnp.concatenate([cols(w_q[l]), cols(w_k[l]), cols(w_v[l])])
    o = cols(w_o[l])
    o = padded(jnp.pad(o, ((0, 0), (0, rows - o.shape[1]), (0, 0))), PIECES)
    gate, up = cols(w_gate[l]), cols(w_up[l])
    gu = jnp.stack([gate.reshape(-1, 2, rows, LANES), up.reshape(-1, 2, rows, LANES)], axis=1).reshape(-1, rows, LANES)
    down = w_down[l].reshape(-1, rows, w_down.shape[2] // LANES, LANES)
    whole = down.shape[2] // PIECES * PIECES
    batches = down[:, :, :whole].reshape(down.shape[0], rows, -1, PIECES, LANES).transpose(2, 0, 3, 1, 4)
    tail = padded(down[:, :, whole:].transpose(2, 0, 1, 3).reshape(-1, rows, LANES), PIECES)
    flat = jnp.concatenate([qkv, o, gu, batches.reshape(-1, rows, LANES), tail])
    return flat.reshape(-1, PIECES, rows, LANES)


def solution(mesh):
    batch_spec = P(("dp", "fsdp"), None, None)
    cache_spec = P(("dp", "fsdp"), None, None, None)
    weight_spec = P(None, "fsdp", None)
    side, nz = math.isqrt(mesh.shape["dp"]), mesh.shape["fsdp"] // 2

    def per_device(x, w_q, w_k, w_v, w_o, w_gate, w_up, w_down, norm_w, qk_norm_w):
        layers, rows, qw = w_q.shape
        _, seq, dm = x.shape
        hd = qk_norm_w.shape[-1]
        heads, ffn = qw // hd, w_gate.shape[2]
        scale = (dm // heads if hd == 128 else hd) ** -0.5
        stacked = (w_q, w_k, w_v, w_o, w_gate, w_up, w_down)
        share = jnp.concatenate([units(rows, l, *stacked) for l in range(layers)])
        ng = share.shape[0]
        tab = jnp.stack([rope_tables(seq, hd, ROPE_BASES[l], ROPE_DIVS[l]) for l in range(layers)])
        ncol, nf = dm // LANES, ffn // (2 * LANES)
        cfg = (side, nz, ng, layers, heads, hd, nf, w_down.shape[1] // rows, scale)
        nsem = 2 * (nz // 2) + 4
        bf, f32 = jnp.bfloat16, jnp.float32
        any_spec, vmem = pl.BlockSpec(memory_space=pl.ANY), pl.BlockSpec(memory_space=pltpu.VMEM)
        out = pl.pallas_call(
            functools.partial(kernel, cfg),
            out_shape=(jax.ShapeDtypeStruct((seq, dm), bf), jax.ShapeDtypeStruct((seq, hd), bf),
                       jax.ShapeDtypeStruct((seq, hd), bf),
                       jax.ShapeDtypeStruct((ng, PIECES, nz, 2 * rows, LANES), bf)),
            in_specs=[any_spec, vmem, vmem, vmem, any_spec],
            out_specs=(any_spec,) * 4,
            scratch_shapes=[
                pltpu.VMEM((seq, dm), bf), pltpu.VMEM((seq, dm), bf), pltpu.VMEM((seq, dm), bf),
                pltpu.VMEM((heads, seq, hd), bf), pltpu.VMEM((seq, hd), bf), pltpu.VMEM((seq, hd), bf),
                pltpu.VMEM((heads, seq, hd), bf),
                pltpu.VMEM((ncol, w_o.shape[1] * 2 * nz, LANES), bf),
                pltpu.VMEM((nf, seq, 2 * LANES), bf),
                pltpu.VMEM((ncol // 2, seq, 2 * LANES), f32),
                pltpu.VMEM((2, PIECES, dm, LANES), bf),
                pltpu.VMEM((2, PIECES, ffn, LANES), bf),
                pltpu.SemaphoreType.DMA((nsem, SLOTS)), pltpu.SemaphoreType.DMA((nsem, SLOTS)),
                pltpu.SemaphoreType.DMA((SLOTS,)), pltpu.SemaphoreType.DMA((2,)), pltpu.SemaphoreType.DMA((1,)),
                pltpu.SemaphoreType.DMA((2,)), pltpu.SemaphoreType.DMA((3,)),
            ],
            compiler_params=pltpu.CompilerParams(
                collective_id=0, has_side_effects=True, vmem_limit_bytes=63 * 1024 * 1024),
        )(x.reshape(seq, dm), norm_w, qk_norm_w, tab, share)
        return out[0][None], out[1][None, :, None], out[2][None, :, None]

    in_specs = (batch_spec,) + (weight_spec,) * 7 + (P(), P())
    return jax.shard_map(per_device, mesh=mesh, in_specs=in_specs, out_specs=(batch_spec, cache_spec, cache_spec), check_vma=False)
```

```python
import functools
import math

import jax
import jax.numpy as jnp
import numpy as np
from jax import lax
from jax.experimental import pallas as pl
from jax.experimental.pallas import tpu as pltpu
from jax.sharding import PartitionSpec as P

WINDOW = 1024
NORM_EPS = 1e-6
ROPE_BASES = (10000.0, 1000000.0)
ROPE_DIVS = (1.0, 8.0)
MESH = pl.DeviceIdType.MESH
LANES = 128
DELTA = 2
SLOTS = 8
NW = 3
AHEAD = 6
PIECES = 4


class Plan:
    def __init__(self, weights):
        w_q, w_k, _, w_o, w_gate, _, w_down = weights
        self.rows, self.ncol = w_q.shape[1], w_o.shape[2] // LANES
        self.nsub = w_down.shape[1] // self.rows
        self.kv = w_q.shape[2] // (PIECES * LANES)
        self.o = self.kv + 1
        self.odd = self.o + self.ncol // PIECES
        self.ffn = self.odd + 2
        self.nf = w_gate.shape[2] // (2 * LANES)
        self.down = self.ffn + self.nf
        self.per = self.down + self.ncol // PIECES * self.nsub
        self.halves = self.per - self.nsub


class Comm:
    def __init__(self, side, nz, layers, weights, g_ref, ssem, rsem, lsem):
        self.plan = Plan(weights)
        self.ng, self.nz, self.w, self.g = layers * self.plan.per, nz, weights, g_ref
        self.ssem, self.rsem, self.lsem = ssem, rsem, lsem
        d, f = lax.axis_index("dp"), lax.axis_index("fsdp")
        self.z, self.c = f // 2, f % 2
        xi, yi = d // side, d % side
        a, b = xi % 2, yi % 2
        self.h = (a + b) % 2
        self.up = {"dp": d, "fsdp": ((self.z + 1) % nz) * 2 + self.c}
        self.down = {"dp": d, "fsdp": ((self.z + nz - 1) % nz) * 2 + self.c}
        self.sib = {"dp": d, "fsdp": self.z * 2 + 1 - self.c}
        self.over_x = {"dp": (xi + 1 - 2 * a) * side + yi, "fsdp": f}
        self.over_y = {"dp": xi * side + yi + 1 - 2 * b, "fsdp": f}
        self.hops = nz // 2
        self.stages = self.hops + 2

    def barrier(self):
        bar = pltpu.get_barrier_semaphore()
        peers = (self.up, self.down, self.sib, self.over_x, self.over_y)
        for peer in peers:
            pl.semaphore_signal(bar, inc=1, device_id=peer, device_id_type=MESH)
        pl.semaphore_wait(bar, len(peers))

    def copies(self, k, g, slot):
        rows, nz, n = self.plan.rows, self.nz, 2 * self.hops
        mine = pl.ds(pl.multiple_of(self.c * rows, 8), rows)

        def remote(i, src, dst, peer):
            return pltpu.make_async_remote_copy(
                src_ref=src, dst_ref=dst, send_sem=self.ssem.at[i, slot], recv_sem=self.rsem.at[i, slot],
                device_id=peer, device_id_type=MESH)

        if k < self.hops:
            half = k == self.hops - 1
            pu = pl.ds(2 * self.h, 1 if half else 2)
            pd = pl.ds(2 * self.h + 1, 1) if half else pu
            su, sd = self.g.at[g, pu, (nz - k) % nz, mine], self.g.at[g, pd, k, mine]
            return [remote(2 * k, su, self.g.at[g, pu, nz - 1 - k, mine], self.up),
                    remote(2 * k + 1, sd, self.g.at[g, pd, k + 1, mine], self.down)]
        rest = pl.ds(1, nz - 1)
        if k == self.hops:
            p = 2 * self.h
            px, py = self.g.at[g, p, rest, mine], self.g.at[g, p + 1, rest, mine]
            return [remote(n, px, px, self.over_x), remote(n + 1, py, py, self.over_y)]
        both = self.g.at[g, :, :, mine]
        return [remote(n + 2, both, both, self.sib)]

    def fetch(self, g):
        pn, rows, slot = self.plan, self.plan.rows, g % SLOTS
        w_q, w_k, w_v, w_o, w_gate, w_up, w_down = self.w
        l = g // pn.per
        i = g - l * pn.per
        every = pl.ds(0, rows)

        def cols(first, n=1):
            return pl.ds(pl.multiple_of(first * LANES, LANES), n * LANES)

        def piece(p, src):
            dst = self.g.at[g, p, 0, pl.ds(pl.multiple_of(self.c * rows, 8), src.shape[0])]
            pltpu.make_async_copy(src, dst, self.lsem.at[p, slot]).start()

        def case(low, high, srcs):
            @pl.when((i >= low) & (i < high))
            def _():
                for p, src in enumerate(srcs()):
                    piece(p, src)

        four = range(PIECES)
        last = pn.ncol - 1
        case(0, pn.kv, lambda: [w_q.at[l, :, cols(PIECES * i + p)] for p in four])
        case(pn.kv, pn.o, lambda: [w.at[l, :, cols(p)] for w in (w_k, w_v) for p in range(2)])
        case(pn.o, pn.odd, lambda: [w_o.at[l, :, cols(PIECES * (i - pn.o) + p)] for p in four])

        def down(r, col):
            return w_down.at[l, pl.ds(pl.multiple_of(r * rows, 8), rows), cols(col)]
        case(pn.odd, pn.odd + 1, lambda: [w_o.at[l, :, cols(last)]] + [down(p, last) for p in range(3)])
        case(pn.odd + 1, pn.ffn, lambda: [down(3 + p, last) for p in range(pn.nsub - 3)])
        case(pn.ffn, pn.down, lambda: [w.at[l, :, cols(2 * (i - pn.ffn) + p)] for w in (w_gate, w_up) for p in range(2)])
        m = i - pn.down
        case(pn.down, pn.halves, lambda: [down(m % pn.nsub, PIECES * (m // pn.nsub) + p) for p in four])
        e = i - pn.halves
        n, col = pn.nsub // 2, last - PIECES
        case(pn.halves, pn.per, lambda: [down(2 * (e % n) + p // 2, col + 2 * (e // n) + p % 2) for p in four])

    def fetched(self, g):
        pn, slot = self.plan, g % SLOTS
        i = g % pn.per
        short = self.w[3].shape[1]

        def case(cond, sizes):
            @pl.when(cond)
            def _():
                for p, n in enumerate(sizes):
                    part = self.g.at[g, p, 0, pl.ds(0, n)]
                    pltpu.make_async_copy(part, part, self.lsem.at[p, slot]).wait()

        full = pn.rows
        case((i < pn.o) | (i >= pn.ffn), [full] * PIECES)
        case((i >= pn.o) & (i < pn.odd), [short] * PIECES)
        case(i == pn.odd, [short] + [full] * 3)
        case(i == pn.odd + 1, [full] * (pn.nsub - 3))

    def tick(self, t):
        slot, old = t % SLOTS, (t + SLOTS - DELTA) % SLOTS

        @pl.when(t < self.ng)
        def _():
            self.fetched(t)
            for cp in self.copies(0, t, slot):
                cp.start()

        @pl.when(t + AHEAD < self.ng)
        def _():
            self.fetch(t + AHEAD)

        for k in range(1, self.stages + 1):
            g = t - DELTA * k

            @pl.when((g >= 0) & (g < self.ng))
            def _(k=k, g=g):
                for cp in self.copies(k - 1, g, old):
                    cp.wait()
                if k < self.stages:
                    for cp in self.copies(k, g, slot):
                        cp.start()

    def ticks(self, first, count):
        def body(i, carry):
            self.tick(first + i)
            return carry
        lax.fori_loop(0, count, body, 0)


def rms(values, gain):
    mean_sq = jnp.mean(values * values, axis=-1, keepdims=True)
    return values * lax.rsqrt(mean_sq + NORM_EPS) * (1.0 + gain)


def rope(values, cos_t, sin_t):
    half = values.shape[-1] // 2
    lo, hi = values[:, :half], values[:, half:]
    return jnp.concatenate([lo * cos_t - hi * sin_t, hi * cos_t + lo * sin_t], axis=-1)


def dot(a, b):
    return jnp.dot(a, b, preferred_element_type=jnp.float32)


def kernel(cfg, x_hbm, nw, qkn, *refs):
    layers = cfg[2]
    tabs, weights, refs = refs[:2 * layers], refs[2 * layers:2 * layers + 7], refs[2 * layers + 7:]
    (xo_hbm, ko_hbm, vo_hbm, g_hbm, xs, hs, x1, qs, ks, vs, at, ob, us, ys, yt, wb, db, dt, tab,
     ssem, rsem, lsem, wsem, osem, dsem, iosem) = refs
    side, nz, layers, scale = cfg
    seq, dm = xs.shape
    heads = qs.shape[0]
    cm = Comm(side, nz, layers, weights, g_hbm, ssem, rsem, lsem)
    pn = cm.plan
    rows, nsub, ncol, nf, per = pn.rows, pn.nsub, pn.ncol, pn.nf, pn.per
    rows_o, rows_d = weights[3].shape[1], weights[6].shape[1]
    def fetch_ahead(g, carry):
        cm.fetch(g)
        return carry
    lax.fori_loop(0, AHEAD, fetch_ahead, 0)
    load_x = pltpu.make_async_copy(x_hbm, xs, iosem.at[0])
    load_x.start()
    for i, tab_hbm in enumerate(tabs):
        pltpu.make_async_copy(tab_hbm, tab.at[i // 2, i % 2], iosem.at[3]).start()
    cm.barrier()
    lead = DELTA * cm.stages + 1
    first = lead + pn.kv
    MB = 256

    def place(rel):
        return (cm.z + rel) % nz

    def load_w(g, slot):
        for rel in range(nz):
            dst = wb.at[slot, :, pl.ds(pl.multiple_of(place(rel) * 2 * rows, 16), 2 * rows), :]
            pltpu.make_async_copy(g_hbm.at[g, :, rel], dst, wsem.at[slot]).start()

    def wait_w(slot):
        pltpu.make_async_copy(wb.at[slot], wb.at[slot], wsem.at[slot]).wait()

    def load_o(base):
        for i in range(pl.cdiv(ncol, PIECES)):
            n = min(PIECES, ncol - PIECES * i)
            for rel in range(nz):
                for c in range(2):
                    src = g_hbm.at[base + pn.o + i, pl.ds(0, n), rel, pl.ds(c * rows, rows_o), :]
                    off = pl.multiple_of((place(rel) * 2 + c) * rows_o, 16)
                    dst = ob.at[pl.ds(PIECES * i, n), pl.ds(off, rows_o), :]
                    pltpu.make_async_copy(src, dst, osem.at[0]).start()

    def wait_o():
        pltpu.make_async_copy(ob, ob, osem.at[0]).wait()

    def load_d(base, k, whole):
        def part(pieces, cols, r, sem):
            for rel in range(nz):
                for c in range(2):
                    src = g_hbm.at[base + pn.down + k, pieces, rel, pl.ds(c * rows, rows), :]
                    off = pl.multiple_of((place(rel) * 2 + c) * rows_d + r * rows, 8)
                    pltpu.make_async_copy(src, db.at[cols, pl.ds(off, rows), :], dsem.at[sem]).start()

        if whole:
            part(pl.ds(0, PIECES), pl.ds(0, PIECES), k, 0)
        else:
            e = k - nsub
            half, n = e // (nsub // 2), e % (nsub // 2)
            for q in range(2):
                part(pl.ds(2 * q, 2), pl.ds(PIECES + 2 * half, 2), 2 * n + q, 1 + half)

    def wait_d(first_col, n, sem):
        part = db.at[pl.ds(first_col, n)]
        pltpu.make_async_copy(part, part, dsem.at[sem]).wait()

    def load_odd(base):
        for r in range(nsub):
            for rel in range(nz):
                for c in range(2):
                    src = g_hbm.at[base + pn.odd + (r + 1) // PIECES, (r + 1) % PIECES, rel, pl.ds(c * rows, rows), :]
                    off = pl.multiple_of((place(rel) * 2 + c) * rows_d + r * rows, 8)
                    pltpu.make_async_copy(src, dt.at[pl.ds(off, rows), :], osem.at[1]).start()

    def wait_odd():
        pltpu.make_async_copy(dt, dt, osem.at[1]).wait()

    def blocks(n, size, body):
        def step(i, carry):
            body(i, pl.ds(pl.multiple_of(i * size, size), size))
            return carry
        lax.fori_loop(0, n // size, step, 0)

    load_x.wait()
    pltpu.make_async_copy(tab, tab, iosem.at[3]).wait()

    def start_up(i, r):
        cm.tick(i)
        hs[r, :] = rms(xs[r, :].astype(jnp.float32), nw[0, pl.ds(0, 1), :]).astype(jnp.bfloat16)
    blocks(seq, MB, start_up)
    begun = seq // MB
    cm.ticks(begun, first - begun)

    def pair(ref, p):
        return jnp.concatenate([ref[2 * p], ref[2 * p + 1]], axis=-1)

    def layer(l, carry):
        base = l * per
        t0 = base + first

        for i in range(pn.kv + 1):
            load_w(base + i, i)

        def head_out(r, acc, which):
            out = rms(acc, qkn[l, pl.ds(which, 1), :])
            return rope(out, tab[l, 0, r, :], tab[l, 1, r, :]).astype(jnp.bfloat16)

        def q_group(i, carry):
            wait_w(i)

            def q_block(j, r):
                for p in range(2):
                    qs[2 * i + p, r, :] = head_out(r, dot(hs[r, :], pair(wb.at[i], p)), 0)
            blocks(seq, MB, q_block)
            cm.tick(t0 + i)
            return carry
        lax.fori_loop(0, pn.kv, q_group, 0)
        wait_w(pn.kv)

        def kv_block(j, r):
            ks[r, :] = head_out(r, dot(hs[r, :], pair(wb.at[pn.kv], 0)), 1)
            vs[r, :] = dot(hs[r, :], pair(wb.at[pn.kv], 1)).astype(jnp.bfloat16)
        blocks(seq, MB, kv_block)
        cm.tick(t0 + pn.kv)
        load_o(base)
        done = pn.kv + 1

        @pl.when(l == layers - 1)
        def _():
            pltpu.make_async_copy(ks, ko_hbm, iosem.at[1]).start()
            pltpu.make_async_copy(vs, vo_hbm, iosem.at[2]).start()

        nb = seq // MB
        for b in range(nb):
            r = pl.ds(b * MB, MB)
            span = (b + 1) * MB
            per_tick = heads if b < nb // 2 else heads // 2

            def one_head(j, b=b, r=r, span=span):
                sc = lax.dot_general(qs[j, r, :], ks[pl.ds(0, span), :], (((1,), (1,)), ((), ())),
                                     preferred_element_type=jnp.float32) * scale
                diff = (b * MB + lax.broadcasted_iota(jnp.int32, sc.shape, 0)
                        - lax.broadcasted_iota(jnp.int32, sc.shape, 1))
                allowed = diff >= 0
                if span > WINDOW:
                    allowed = allowed & ((diff < WINDOW) | (l > 0))
                sc = jnp.where(allowed, sc, -1e30)
                e = jnp.exp(sc - jnp.max(sc, axis=-1, keepdims=True))
                probs = (e * (1.0 / jnp.sum(e, axis=-1, keepdims=True))).astype(jnp.bfloat16)
                at[j, r, :] = dot(probs, vs[pl.ds(0, span), :]).astype(jnp.bfloat16)

            def some_heads(i, carry, per_tick=per_tick, done=done, one_head=one_head):
                def body(j, carry):
                    one_head(i * per_tick + j)
                    return carry
                lax.fori_loop(0, per_tick, body, 0)
                cm.tick(t0 + done + i)
                return carry
            lax.fori_loop(0, heads // per_tick, some_heads, 0)
            done += heads // per_tick

        for j in range(2):
            load_w(base + pn.ffn + j, j)
        load_odd(base)
        wait_o()

        def o_block(i, r):
            lhs = jnp.concatenate([at[j, r, :] for j in range(heads)], axis=-1)
            parts = [dot(lhs, pair(ob, p)) for p in range(ncol // 2)]
            if ncol % 2:
                parts.append(dot(lhs, ob[ncol - 1]))
            proj = jnp.concatenate(parts, axis=-1)
            res = (xs[r, :].astype(jnp.float32) + rms(proj, nw[l, pl.ds(1, 1), :])).astype(jnp.bfloat16)
            x1[r, :] = res
            hs[r, :] = rms(res.astype(jnp.float32), nw[l, pl.ds(2, 1), :]).astype(jnp.bfloat16)
        nb = seq // MB

        def o_step(i, carry):
            for m in range(2):
                o_block(0, pl.ds(pl.multiple_of((2 * i + m) * MB, MB), MB))
            cm.tick(t0 + done + i)
            return carry
        lax.fori_loop(0, nb // 2, o_step, 0)
        done += nb // 2

        def gu(j, more=True):
            slot = j % NW
            if more:
                load_w(base + pn.ffn + j + 2, (j + 2) % NW)
            wait_w(slot)

            def block(i, r):
                gate, up = dot(hs[r, :], pair(wb.at[slot], 0)), dot(hs[r, :], pair(wb.at[slot], 1))
                us[j, r, :] = (jax.nn.gelu(gate, approximate=True) * up).astype(jnp.bfloat16)
            blocks(seq, 2 * MB, block)

        fast = first + done - 2 - pn.ffn - lead

        def two(i, carry):
            gu(2 * i)
            gu(2 * i + 1)
            cm.tick(t0 + done + i)
            return carry
        lax.fori_loop(0, fast, two, 0)
        done += fast

        def one(i, carry):
            gu(2 * fast + i)
            cm.tick(t0 + done + i)
            return carry
        singles = nf - 2 - 2 * fast
        lax.fori_loop(0, singles, one, 0)
        done += singles
        def end(i, carry):
            gu(nf - 2 + i, more=False)
            cm.tick(t0 + done + i)
            return carry
        lax.fori_loop(0, 2, end, 0)
        done += 2

        def lhs_u(r):
            return jnp.concatenate([us[j, r, :] for j in range(nf)], axis=-1)

        def d_step(i):
            p, m = i // nb, i % nb
            r = pl.ds(pl.multiple_of(m * MB, MB), MB)
            ys[p, r, :] = dot(lhs_u(r), jnp.concatenate([db[2 * p], db[2 * p + 1]], axis=-1))

        def odd(i):
            r = pl.ds(pl.multiple_of(i * MB, MB), MB)
            yt[r, :] = dot(lhs_u(r), dt[...])

        wait_odd()
        ready = first + done - lead - pn.down + 1
        def load_whole(k, carry):
            load_d(base, k, True)
            return carry
        lax.fori_loop(0, ready, load_whole, 0)

        def odd_step(i, carry):
            odd(i)
            cm.tick(t0 + done + i)
            load_d(base, ready + i, True)
            return carry
        lax.fori_loop(0, nsub - ready, odd_step, 0)
        done += nsub - ready
        for i in range(nsub - ready, nb):
            odd(i)
        wait_d(0, PIECES, 0)

        def d_pair(i, carry):
            @pl.when(i == nb)
            def _():
                wait_d(PIECES, 2, 1)
            d_step(2 * i)
            d_step(2 * i + 1)
            cm.tick(t0 + done + i)
            load_d(base, nsub + i, False)
            return carry
        lax.fori_loop(0, nsub, d_pair, 0)
        done += nsub
        wait_d(PIECES + 2, 2, 2)

        def fin(i, r):
            parts = [ys[p, r, :] for p in range(ncol // 2 - 1)]
            parts += [dot(lhs_u(r), pair(db, ncol // 2 - 1)), yt[r, :]]
            res = (x1[r, :].astype(jnp.float32) + rms(jnp.concatenate(parts, axis=-1), nw[l, pl.ds(3, 1), :])).astype(jnp.bfloat16)
            xs[r, :] = res
            nxt = jnp.minimum(l + 1, layers - 1)
            hs[r, :] = rms(res.astype(jnp.float32), nw[nxt, pl.ds(0, 1), :]).astype(jnp.bfloat16)
        left = per - done

        def fin_tick(i, carry):
            fin(i, pl.ds(pl.multiple_of(i * MB, MB), MB))
            cm.tick(t0 + done + i)
            return carry
        lax.fori_loop(0, min(left, nb), fin_tick, 0)
        for i in range(min(left, nb), nb):
            fin(i, pl.ds(i * MB, MB))
        cm.ticks(t0 + done + nb, left - nb)
        return carry

    lax.fori_loop(0, layers, layer, 0)
    out = pltpu.make_async_copy(xs, xo_hbm, iosem.at[0])
    out.start()
    pltpu.make_async_copy(ks, ko_hbm, iosem.at[1]).wait()
    pltpu.make_async_copy(vs, vo_hbm, iosem.at[2]).wait()
    out.wait()


def rope_tables(seq_len, head_dim, rope_base, pos_div):
    half_dim = head_dim // 2
    inv_freq = (rope_base ** (-2.0 * np.arange(half_dim) / head_dim)).astype(np.float32)
    positions = jnp.arange(seq_len, dtype=jnp.float32) / pos_div
    angles = positions[:, None] * jnp.asarray(inv_freq)[None, :]
    return jnp.cos(angles), jnp.sin(angles)


def solution(mesh):
    batch_spec = P(("dp", "fsdp"), None, None)
    cache_spec = P(("dp", "fsdp"), None, None, None)
    weight_spec = P(None, "fsdp", None)
    side, nz = math.isqrt(mesh.shape["dp"]), mesh.shape["fsdp"] // 2

    def per_device(x, w_q, w_k, w_v, w_o, w_gate, w_up, w_down, norm_w, qk_norm_w):
        layers, rows, qw = w_q.shape
        _, seq, dm = x.shape
        hd = qk_norm_w.shape[-1]
        heads, ffn, ncol, nf = qw // hd, w_gate.shape[2], dm // LANES, w_gate.shape[2] // (2 * LANES)
        scale = (dm // heads if hd == 128 else hd) ** -0.5
        weights = (w_q, w_k, w_v, w_o, w_gate, w_up, w_down)
        ng = layers * Plan(weights).per
        tabs = [t for l in range(layers) for t in rope_tables(seq, hd, ROPE_BASES[l], ROPE_DIVS[l])]
        cfg = (side, nz, layers, scale)
        nsem = 2 * (nz // 2) + 3
        bf, f32 = jnp.bfloat16, jnp.float32
        any_spec, vmem = pl.BlockSpec(memory_space=pl.ANY), pl.BlockSpec(memory_space=pltpu.VMEM)
        out = pl.pallas_call(
            functools.partial(kernel, cfg),
            out_shape=(jax.ShapeDtypeStruct((seq, dm), bf), jax.ShapeDtypeStruct((seq, hd), bf),
                       jax.ShapeDtypeStruct((seq, hd), bf),
                       jax.ShapeDtypeStruct((ng, PIECES, nz, 2 * rows, LANES), bf)),
            in_specs=[any_spec, vmem, vmem] + [any_spec] * (len(tabs) + len(weights)),
            out_specs=(any_spec,) * 4,
            scratch_shapes=[
                pltpu.VMEM((seq, dm), bf), pltpu.VMEM((seq, dm), bf), pltpu.VMEM((seq, dm), bf),
                pltpu.VMEM((heads, seq, hd), bf), pltpu.VMEM((seq, hd), bf), pltpu.VMEM((seq, hd), bf),
                pltpu.VMEM((heads, seq, hd), bf),
                pltpu.VMEM((ncol, w_o.shape[1] * 2 * nz, LANES), bf),
                pltpu.VMEM((nf, seq, 2 * LANES), bf),
                pltpu.VMEM((ncol // 2, seq, 2 * LANES), f32),
                pltpu.VMEM((seq, LANES), f32),
                pltpu.VMEM((NW, PIECES, dm, LANES), bf),
                pltpu.VMEM((ncol - 1, ffn, LANES), bf),
                pltpu.VMEM((ffn, LANES), bf),
                pltpu.VMEM((layers, 2, seq, hd // 2), f32),
                pltpu.SemaphoreType.DMA((nsem, SLOTS)), pltpu.SemaphoreType.DMA((nsem, SLOTS)),
                pltpu.SemaphoreType.DMA((PIECES, SLOTS)), pltpu.SemaphoreType.DMA((NW,)), pltpu.SemaphoreType.DMA((2,)),
                pltpu.SemaphoreType.DMA((3,)), pltpu.SemaphoreType.DMA((4,)),
            ],
            compiler_params=pltpu.CompilerParams(
                collective_id=0, has_side_effects=True, vmem_limit_bytes=63 * 1024 * 1024),
        )(x.reshape(seq, dm), norm_w, qk_norm_w, *tabs, *weights)
        return out[0][None], out[1][None, :, None], out[2][None, :, None]

    in_specs = (batch_spec,) + (weight_spec,) * 7 + (P(), P())
    return jax.shard_map(per_device, mesh=mesh, in_specs=in_specs, out_specs=(batch_spec, cache_spec, cache_spec), check_vma=False)
```
